16 devices in a mesh: w: 2 (over z), h: 8 (over y, x, core).
Axes of the slice: x: 2, y: 2, z: 2, core: 2. Of those that a mesh axis runs over, the one named last changes fastest.
Arguments:
- x: bfloat16 [1, 64, 512, 640], P(None, 'h', 'w')
- w1: bfloat16 [3, 3, 640, 640], replicated
- gamma: float32 [640], replicated
- beta: float32 [640], replicated
- w2: bfloat16 [3, 3, 640, 640], replicated
- g: bfloat16 [1, 64, 512, 640], P(None, 'h', 'w')
Outputs:
- output 1: bfloat16 [1, 64, 512, 640], P(None, 'h', 'w')
- output 2: bfloat16 [1, 64, 512, 640], P(None, 'h', 'w')
- output 3: float32 [3, 3, 640, 640], replicated
- output 4: float32 [3, 3, 640, 640], replicated
- output 5: float32 [640], replicated
- output 6: float32 [640], replicated
All inputs are finite; a program needn't handle non-finite values.
Results may differ from the reference program's by a relative error of at most 0.00136563.
Values are sent between devices in bfloat16 or wider.
A program may use at most 1 GiB of HBM per device.

```python
import jax
import jax.numpy as jnp
from jax import lax

B = 1
C = 640
GROUPS = 32
TH = 8
TW = 256
HT = 8
WT = 2
HS = HT * TH
WS = WT * TW
DN = ('NHWC', 'HWIO', 'NHWC')


def setup_inputs(seed: int = 0) -> dict:
    ks = jax.random.split(jax.random.PRNGKey(seed), 6)
    rows = jnp.arange(HS)
    cols = jnp.arange(WS)
    xs = (0.5 + 1.5 * rows / HS)[None, :, None, None]
    x = (jax.random.normal(ks[0], (B, HS, WS, C), jnp.float32) * xs).astype(jnp.bfloat16)
    std = (9 * C) ** -0.5
    w1 = (jax.random.normal(ks[1], (3, 3, C, C), jnp.float32) * std).astype(jnp.bfloat16)
    gamma = 1.0 + 0.3 * jax.random.normal(ks[2], (C,), jnp.float32)
    beta = 0.3 * jax.random.normal(ks[3], (C,), jnp.float32)
    w2 = (jax.random.normal(ks[4], (3, 3, C, C), jnp.float32) * std).astype(jnp.bfloat16)
    edge = ((rows % TH == 0) | (rows % TH == TH - 1))[:, None] | ((cols % TW == 0) | (cols % TW == TW - 1))[None, :]
    gs = jnp.where(edge, 3.0, 1.0)[None, :, :, None]
    g = (jax.random.normal(ks[5], (B, HS, WS, C), jnp.float32) * gs).astype(jnp.bfloat16)
    return {'x': x, 'w1': w1, 'gamma': gamma, 'beta': beta, 'w2': w2, 'g': g}


def _conv(u, w):
    return lax.conv_general_dilated(u.astype(jnp.float32), w.astype(jnp.float32), (1, 1), 'SAME', dimension_numbers=DN)


def _conv_t(v, w):
    return _conv(v, jnp.flip(w, (0, 1)).transpose(0, 1, 3, 2))


def _wgrad(u, v):
    up = jnp.pad(u.astype(jnp.float32), ((0, 0), (1, 1), (1, 1), (0, 0)))
    v32 = v.astype(jnp.float32)
    h, w = v.shape[1], v.shape[2]
    return jnp.stack([jnp.stack([jnp.einsum('bhwc,bhwo->co', up[:, a:a + h, b:b + w], v32) for b in range(3)]) for a in range(3)])


def _norm_act(a, gamma, beta):
    nb, h, w, c = a.shape
    ag = a.reshape(nb, h, w, GROUPS, c // GROUPS)
    mean = ag.mean(axis=(1, 2, 4), keepdims=True)
    var = ((ag - mean) ** 2).mean(axis=(1, 2, 4), keepdims=True)
    n = ((ag - mean) * lax.rsqrt(var + 1e-5)).reshape(a.shape) * gamma + beta
    return jax.nn.gelu(n, approximate=True)


def reference(x, w1, gamma, beta, w2, g):
    a = _conv(x, w1).astype(jnp.bfloat16).astype(jnp.float32)
    zf, vjp = jax.vjp(_norm_act, a, gamma, beta)
    z = zf.astype(jnp.bfloat16)
    y = (_conv(z, w2) + x.astype(jnp.float32)).astype(jnp.bfloat16)
    dz = _conv_t(g, w2)
    dw2 = _wgrad(z, g)
    da, dgamma, dbeta = vjp(dz)
    da = da.astype(jnp.bfloat16)
    dx = (_conv_t(da, w1) + g.astype(jnp.float32)).astype(jnp.bfloat16)
    dw1 = _wgrad(x, da)
    return y, dx, dw1, dw2, dgamma, dbeta
```

```python
import jax
import jax.numpy as jnp
from jax import lax
from jax.experimental import pallas as pl
from jax.experimental.pallas import tpu as pltpu
from jax.sharding import PartitionSpec as P

GROUPS = 32
EPS = 1e-5
MESH = pl.DeviceIdType.MESH
F32 = jnp.float32
BF = jnp.bfloat16
ANY = pl.BlockSpec(memory_space=pl.ANY)
VM = pl.BlockSpec(memory_space=pltpu.VMEM)
TH, TW, C = 8, 256, 640
PIX = TH * TW
GC = 0.7978845608028654
GA = 0.044715


def _gelu_parts(n):
    n2 = n * n
    t = jnp.tanh(GC * n * (1.0 + GA * n2))
    return n2, t


def _halo_scratch():
    return [pltpu.VMEM((16, C), BF), pltpu.VMEM((3, 16, C), BF), pltpu.VMEM((2, TW, C), BF), pltpu.VMEM((16, C), F32), pltpu.VMEM((10, 8, C), F32),
            pltpu.SemaphoreType.DMA((5,)), pltpu.SemaphoreType.DMA((5,))]


class _Halo:
    def __init__(self, src, scratch):
        self.src = src
        self.edge, self.cols, self.rows, self.colf, self.colp, self.ssem, self.rsem = scratch
        self.w, self.h = lax.axis_index('w'), lax.axis_index('h')

    def _copy(self, i, a, b, dev):
        return pltpu.make_async_remote_copy(src_ref=a, dst_ref=b, send_sem=self.ssem.at[i], recv_sem=self.rsem.at[i], device_id=dev, device_id_type=MESH)

    def _copies(self):
        w, h = self.w, self.h
        return (self._copy(0, self.edge, self.cols.at[1], (1 - w, h)),
                self._copy(1, self.edge, self.cols.at[0], (1 - w, h + 1)),
                self._copy(2, self.edge, self.cols.at[2], (1 - w, h - 1)),
                self._copy(3, self.src.at[pl.ds(PIX - TW, TW)], self.rows.at[0], (w, h + 1)),
                self._copy(4, self.src.at[pl.ds(0, TW)], self.rows.at[1], (w, h - 1)))

    def start(self, nh=8):
        w, h = self.w, self.h
        c = self._copies()

        @pl.when(h < nh - 1)
        def _():
            c[3].start()

        @pl.when(h > 0)
        def _():
            c[4].start()
        for i in range(TH):
            first = self.src[i * TW:i * TW + 16, :].astype(F32)[0:1]
            last = self.src[i * TW + TW - 16:i * TW + TW, :].astype(F32)[15:16]
            self.colf[i:i + 1, :] = jnp.where(w == 0, last, first)
        self.colf[8:16, :] = jnp.zeros((8, C), F32)
        self.edge[...] = self.colf[...].astype(BF)
        c[0].start()

        @pl.when(h < nh - 1)
        def _():
            c[1].start()

        @pl.when(h > 0)
        def _():
            c[2].start()

        @pl.when(h == 0)
        def _():
            self.rows[0] = jnp.zeros((TW, C), BF)
            self.cols[0] = jnp.zeros((16, C), BF)

        @pl.when(h == nh - 1)
        def _():
            self.rows[1] = jnp.zeros((TW, C), BF)
            self.cols[2] = jnp.zeros((16, C), BF)

    def wait_cols(self, nh=8):
        h = self.h
        c = self._copies()
        c[0].wait()

        @pl.when(h < nh - 1)
        def _():
            c[1].wait_send()
            c[2].wait_recv()

        @pl.when(h > 0)
        def _():
            c[2].wait_send()
            c[1].wait_recv()
        self.colp[0, 0:1, :] = self.cols[0].astype(F32)[7:8]
        mine = self.cols[1].astype(F32)
        for i in range(TH):
            self.colp[i + 1, 0:1, :] = mine[i:i + 1]
        self.colp[9, 0:1, :] = self.cols[2].astype(F32)[0:1]

    def wait_rows(self, nh=8):
        h = self.h
        c = self._copies()

        @pl.when(h < nh - 1)
        def _():
            c[3].wait_send()
            c[4].wait_recv()

        @pl.when(h > 0)
        def _():
            c[4].wait_send()
            c[3].wait_recv()

    def row(self, cat, r, load):
        w = self.w
        ids = lax.broadcasted_iota(jnp.int32, (TW, 128), 0)
        out = pl.ds(r * TW if isinstance(r, int) else pl.multiple_of(r * TW, TW), TW)
        for k in range(C // 128):
            s = slice(k * 128, k * 128 + 128)
            x = load(s)
            xf = x.astype(F32)
            p = self.colp[r, 0:1, s]
            pl_ = jnp.where(w == 1, p, 0.0)
            pr = jnp.where(w == 0, p, 0.0)
            cat[out, s] = jnp.where(ids == 0, pl_, pltpu.roll(xf, 1, 0)).astype(BF)
            cat[out, C + k * 128:C + k * 128 + 128] = x
            cat[out, 2 * C + k * 128:2 * C + k * 128 + 128] = jnp.where(ids == TW - 1, pr, pltpu.roll(xf, TW - 1, 0)).astype(BF)

    def center(self, cat, r):
        o = pl.multiple_of((r - 1) * TW, TW)
        self.row(cat, r, lambda s: self.src[pl.ds(o, TW), s])

    def borders(self, cat):
        self.row(cat, 0, lambda s: self.rows[0, :, s])
        self.row(cat, TH + 1, lambda s: self.rows[1, :, s])


def _exchange(buf, ssem, rsem, rows, nh=8, nw=2):
    w, h = lax.axis_index('w'), lax.axis_index('h')
    me = w * nh + h
    n = nh * nw
    copies = []
    for d in range(1, n):
        to = lax.rem(me + d, n)
        copies.append(pltpu.make_async_remote_copy(
            src_ref=buf.at[0], dst_ref=buf.at[d], send_sem=ssem.at[d], recv_sem=rsem.at[d],
            device_id=(to // nh, lax.rem(to, nh)), device_id_type=MESH))
    for c in copies:
        c.start()
    return copies


def _exchange_sum(buf, copies, nh=8, nw=2):
    w, h = lax.axis_index('w'), lax.axis_index('h')
    me = w * nh + h
    n = nh * nw
    for c in copies:
        c.wait()
    total = None
    for src in range(n):
        v = buf[lax.rem(me - src + n, n)]
        total = v if total is None else total + v
    return total


def _group_mats():
    cg = C // GROUPS
    ch = lax.broadcasted_iota(jnp.int32, (C, 128), 0)
    gr = lax.broadcasted_iota(jnp.int32, (C, 128), 1) * cg
    down = jnp.where((ch >= gr) & (ch < gr + cg), 1.0, 0.0).astype(F32)
    ch = lax.broadcasted_iota(jnp.int32, (128, C), 1)
    gr = lax.broadcasted_iota(jnp.int32, (128, C), 0) * cg
    up = jnp.where((ch >= gr) & (ch < gr + cg), 1.0, 0.0).astype(F32)
    return down, up


def _dotf(a, b):
    return jnp.dot(a, b, preferred_element_type=F32, precision=lax.Precision.HIGHEST)


def _conv(cat, w, m0, mb):
    acc = None
    for a in range(3):
        d = jnp.dot(cat[pl.ds(pl.multiple_of(m0 + a * TW, TW), mb), :], w[a], preferred_element_type=F32)
        acc = d if acc is None else acc + d
    return acc


def _conv_t(cat, w, m0, mb):
    acc = None
    for a in range(3):
        rows = pl.ds(pl.multiple_of(m0 + a * TW, TW), mb)
        for b in range(3):
            d = lax.dot_general(cat[rows, b * C:b * C + C], w[2 - a, (2 - b) * C:(2 - b) * C + C, :],
                                (((1,), (1,)), ((), ())), preferred_element_type=F32)
            acc = d if acc is None else acc + d
    return acc


def _k1(cnt, x, w1, g, gamma, beta, gcat_o, a_o, z_o, zt_o, stat_o,
        xv, gv, wv, cat, gcat, av, zv, ztv, sums, ebuf, ess, ers, dsem, *hs):
    n = len(hs) // 2
    hx, hg = _Halo(xv, hs[:n]), _Halo(gv, hs[n:])
    cx = pltpu.make_async_copy(x, xv, dsem.at[0])
    cg_ = pltpu.make_async_copy(g, gv, dsem.at[1])
    cw = pltpu.make_async_copy(w1, wv, dsem.at[2])
    cx.start()
    cg_.start()
    cw.start()
    cx.wait()
    hx.start()
    cg_.wait()
    hg.start()
    sums[...] = jnp.zeros_like(sums)
    hx.wait_cols()

    @pl.loop(1, TH + 1)
    def _(r):
        hx.center(cat, r)
    hx.wait_rows()
    hx.borders(cat)
    hg.wait_cols()
    cw.wait()

    @pl.loop(0, 4)
    def _(i):
        m0 = pl.multiple_of(i * 512, 512)
        a = _conv(cat, wv, m0, 512).astype(BF)
        av[pl.ds(m0, 512), :] = a
        af = a.astype(F32)
        sums[0:1, :] += jnp.sum(af, axis=0, keepdims=True)
        sums[1:2, :] += jnp.sum(af * af, axis=0, keepdims=True)
        hg.center(gcat, 2 * i + 1)
        hg.center(gcat, 2 * i + 2)
    ca = pltpu.make_async_copy(av, a_o, dsem.at[3])
    ca.start()
    down, up = _group_mats()
    ebuf[0] = _dotf(sums[...], down)
    copies = _exchange(ebuf, ess, ers, 8)
    hg.wait_rows()
    hg.borders(gcat)
    cgo = pltpu.make_async_copy(gcat, gcat_o, dsem.at[4])
    cgo.start()
    tot = _exchange_sum(ebuf, copies) * (1.0 / cnt)
    mean_g = tot[0:1]
    rstd_g = lax.rsqrt(tot[1:2] - mean_g * mean_g + EPS)
    row = lax.broadcasted_iota(jnp.int32, (8, 128), 0)
    st = jnp.where(row == 0, mean_g, jnp.where(row == 1, rstd_g, 0.0))
    st = _dotf(st, up)
    stat_o[...] = st
    sums[...] = st

    @pl.loop(0, 8)
    def _(i):
        m0 = pl.multiple_of(i * TW, TW)
        for k in range(C // 128):
            s = slice(k * 128, k * 128 + 128)
            xh = (av[pl.ds(m0, TW), s].astype(F32) - sums[0:1, s]) * sums[1:2, s]
            nn = xh * gamma[:, s] + beta[:, s]
            _, t = _gelu_parts(nn)
            z = nn * (0.5 * (1.0 + t))
            zv[pl.ds(m0, TW), s] = z.astype(BF)
            ztv[s, pl.ds(m0, TW)] = z.T.astype(BF)
    cz = pltpu.make_async_copy(zv, z_o, dsem.at[5])
    czt = pltpu.make_async_copy(ztv, zt_o, dsem.at[6])
    cz.start()
    czt.start()
    ca.wait()
    cgo.wait()
    cz.wait()
    czt.wait()


def _wgrad_block(lt, cat, a, c0):
    rows = pl.ds(pl.multiple_of(c0, 32), 160)
    return jnp.dot(lt[rows, :], cat[pl.ds(pl.multiple_of((2 - a) * TW, TW), PIX), :], preferred_element_type=F32)


def _k2(cnt, gcat_i, zt_i, a_i, stat, gamma, beta, w2, dw_o, da_o, t_o,
        cat, lt, av, wv, dn, blk, sums, ebuf, ess, ers, dsem, bsem):
    ins = [pltpu.make_async_copy(s, d, dsem.at[i]) for i, (s, d) in enumerate(((zt_i, lt), (gcat_i, cat), (w2, wv), (a_i, av)))]
    for c in ins:
        c.start()
    sums[...] = jnp.zeros_like(sums)
    ins[0].wait()
    ins[1].wait()

    def out(j, slot):
        a, q = j // 4, lax.rem(j, 4)
        return pltpu.make_async_copy(blk.at[slot], dw_o.at[a, :, pl.ds(pl.multiple_of(q * 160, 32), 160), :], bsem.at[slot])

    @pl.loop(0, 12)
    def _(j):
        a, q = j // 4, lax.rem(j, 4)
        slot = lax.rem(j, 2)

        @pl.when(j >= 2)
        def _():
            out(j - 2, slot).wait()
        acc = _wgrad_block(lt, cat, a, q * 160)
        for b in range(3):
            blk[slot, b] = acc[:, (2 - b) * C:(2 - b) * C + C]
        out(j, slot).start()
    ins[2].wait()
    ins[3].wait()

    @pl.loop(0, 4)
    def _(i):
        m0 = pl.multiple_of(i * 512, 512)
        dz = _conv_t(cat, wv, m0, 512)
        xh = (av[pl.ds(m0, 512), :].astype(F32) - stat[0:1, :]) * stat[1:2, :]
        nn = xh * gamma[...] + beta[...]
        n2, t = _gelu_parts(nn)
        d = dz * (0.5 * (1.0 + t) + (0.5 * GC) * nn * (1.0 - t * t) * (1.0 + (3.0 * GA) * n2))
        dn[pl.ds(m0, 512), :] = d
        sums[0:1, :] += jnp.sum(d * xh, axis=0, keepdims=True)
        sums[1:2, :] += jnp.sum(d, axis=0, keepdims=True)
    for s in range(2):
        for k in range(5):
            ebuf[0, s * 8 + k:s * 8 + k + 1, :] = sums[s:s + 1, k * 128:k * 128 + 128]
        ebuf[0, s * 8 + 5:s * 8 + 8, :] = jnp.zeros((3, 128), F32)
    copies = _exchange(ebuf, ess, ers, 16)
    out(10, 0).wait()
    out(11, 1).wait()
    tot = _exchange_sum(ebuf, copies)
    for s in range(2):
        for k in range(5):
            sums[s:s + 1, k * 128:k * 128 + 128] = tot[s * 8 + k:s * 8 + k + 1, :]
    t_o[...] = sums[...]
    down, up = _group_mats()
    u = _dotf(_dotf(sums[...] * gamma[...], down) * (1.0 / cnt), up)
    sums[...] = u

    @pl.loop(0, 8)
    def _(i):
        m = pl.ds(pl.multiple_of(i * TW, TW), TW)
        for k in range(C // 128):
            s = slice(k * 128, k * 128 + 128)
            xh = (av[m, s].astype(F32) - stat[0:1, s]) * stat[1:2, s]
            v = stat[1:2, s] * (dn[m, s] * gamma[:, s] - sums[1:2, s] - xh * sums[0:1, s])
            av[m, s] = v.astype(BF)
    co = pltpu.make_async_copy(av, da_o, dsem.at[0])
    co.start()
    co.wait()


def _k3(x, z, da, g, w1, w2, dw_o, y_o, dx_o, xv, zv, dav, gv, lt, wv, w2v, cat, blk, ob, dsem, bsem, *hs):
    n = len(hs) // 2
    hd, hz = _Halo(dav, hs[:n]), _Halo(zv, hs[n:])
    ins = [pltpu.make_async_copy(s, d, dsem.at[i]) for i, (s, d) in enumerate(((da, dav), (x, xv), (z, zv), (w1, wv), (g, gv), (w2, w2v)))]
    for c in ins:
        c.start()
    ins[0].wait()
    hd.start()
    ins[2].wait()
    hz.start()
    ins[1].wait()

    @pl.loop(0, 8)
    def _(i):
        m = pl.ds(pl.multiple_of(i * TW, TW), TW)
        for k in range(C // 128):
            s = slice(k * 128, k * 128 + 128)
            lt[s, m] = xv[m, s].astype(F32).T.astype(BF)
    hd.wait_cols()

    @pl.loop(1, TH + 1)
    def _(r):
        hd.center(cat, r)
    hd.wait_rows()
    hd.borders(cat)

    def out(j, slot):
        a, q = j // 4, lax.rem(j, 4)
        return pltpu.make_async_copy(blk.at[slot], dw_o.at[a, :, pl.ds(pl.multiple_of(q * 160, 32), 160), :], bsem.at[slot])

    @pl.loop(0, 12)
    def _(j):
        a, q = j // 4, lax.rem(j, 4)
        slot = lax.rem(j, 2)

        @pl.when(j >= 2)
        def _():
            out(j - 2, slot).wait()
        acc = _wgrad_block(lt, cat, a, q * 160)
        for b in range(3):
            blk[slot, b] = acc[:, (2 - b) * C:(2 - b) * C + C]
        out(j, slot).start()
    out(10, 0).wait()
    out(11, 1).wait()
    ins[3].wait()
    ins[4].wait()

    @pl.loop(0, 4)
    def _(i):
        m = pl.ds(pl.multiple_of(i * 512, 512), 512)
        ob[m, :] = (_conv_t(cat, wv, i * 512, 512) + gv[m, :].astype(F32)).astype(BF)
    c1 = pltpu.make_async_copy(ob, dx_o, dsem.at[0])
    c1.start()
    hz.wait_cols()

    @pl.loop(1, TH + 1)
    def _(r):
        hz.center(cat, r)
    hz.wait_rows()
    hz.borders(cat)
    ins[5].wait()
    c1.wait()

    @pl.loop(0, 4)
    def _(i):
        m = pl.ds(pl.multiple_of(i * 512, 512), 512)
        ob[m, :] = (_conv(cat, w2v, i * 512, 512) + xv[m, :].astype(F32)).astype(BF)
    c2 = pltpu.make_async_copy(ob, y_o, dsem.at[1])
    c2.start()
    c2.wait()


def _params(**kw):
    return pltpu.CompilerParams(has_side_effects=True, vmem_limit_bytes=64 * 2**20 - 65536, **kw)


def solution(mesh):
    tile = P(None, 'h', 'w', None)
    cnt = float(TH * TW * 16 * (C // GROUPS))
    sds = jax.ShapeDtypeStruct
    DMA = pltpu.SemaphoreType.DMA
    V = pltpu.VMEM

    def body(x, w1, gamma, beta, w2, g):
        x2, g2 = x.reshape(PIX, C), g.reshape(PIX, C)
        w1r, w2r = w1.reshape(3, 3 * C, C), w2.reshape(3, 3 * C, C)
        ga, be = gamma.reshape(1, C), beta.reshape(1, C)
        gcat, a, z, zt, stat = pl.pallas_call(
            lambda *r: _k1(cnt, *r),
            out_shape=[sds((10 * TW, 3 * C), BF), sds((PIX, C), BF), sds((PIX, C), BF), sds((C, PIX), BF), sds((8, C), F32)],
            in_specs=[ANY, ANY, ANY, VM, VM], out_specs=[ANY, ANY, ANY, ANY, VM],
            scratch_shapes=[V((PIX, C), BF), V((PIX, C), BF), V((3, 3 * C, C), BF), V((10 * TW, 3 * C), BF), V((10 * TW, 3 * C), BF),
                            V((PIX, C), BF), V((PIX, C), BF), V((C, PIX), BF), V((8, C), F32), V((16, 8, 128), F32), DMA((16,)), DMA((16,)), DMA((8,))]
            + _halo_scratch() + _halo_scratch(),
            compiler_params=_params(), name='k1')(x2, w1r, g2, ga, be)
        dw2p, da, t = pl.pallas_call(
            lambda *r: _k2(cnt, *r),
            out_shape=[sds((3, 3, C, C), F32), sds((PIX, C), BF), sds((8, C), F32)],
            in_specs=[ANY, ANY, ANY, VM, VM, VM, ANY], out_specs=[ANY, ANY, VM],
            scratch_shapes=[V((10 * TW, 3 * C), BF), V((C, PIX), BF), V((PIX, C), BF), V((3, 3 * C, C), BF), V((PIX, C), F32),
                            V((2, 3, 160, C), F32), V((8, C), F32), V((16, 16, 128), F32), DMA((16,)), DMA((16,)), DMA((8,)), DMA((2,))],
            compiler_params=_params(), name='k2')(gcat, zt, a, stat, ga, be, w2r)
        dw1p, y, dx = pl.pallas_call(
            _k3,
            out_shape=[sds((3, 3, C, C), F32), sds((PIX, C), BF), sds((PIX, C), BF)],
            in_specs=[ANY] * 6, out_specs=[ANY, ANY, ANY],
            scratch_shapes=[V((PIX, C), BF)] * 4 + [V((C, PIX), BF), V((3, 3 * C, C), BF), V((3, 3 * C, C), BF), V((10 * TW, 3 * C), BF),
                            V((2, 3, 160, C), F32), V((PIX, C), BF), DMA((8,)), DMA((2,))]
            + _halo_scratch() + _halo_scratch(),
            compiler_params=_params(), name='k3')(x2, z, da, g2, w1r, w2r)
        dw2 = lax.psum(dw2p, ('h', 'w'))
        dw1 = lax.psum(dw1p, ('h', 'w'))
        return y.reshape(x.shape), dx.reshape(x.shape), dw1, dw2, t[0], t[1]

    return jax.shard_map(body, mesh=mesh, in_specs=(tile, P(), P(), P(), P(), tile), out_specs=(tile, tile, P(), P(), P(), P()), check_vma=False)
```

```python
import jax
import jax.numpy as jnp
from jax import lax
from jax.experimental import pallas as pl
from jax.experimental.pallas import tpu as pltpu
from jax.sharding import PartitionSpec as P

GROUPS = 32
EPS = 1e-5
MESH = pl.DeviceIdType.MESH
F32 = jnp.float32
BF = jnp.bfloat16
ANY = pl.BlockSpec(memory_space=pl.ANY)
VM = pl.BlockSpec(memory_space=pltpu.VMEM)
TH, TW, C = 8, 256, 640
PIX = TH * TW
GC = 0.7978845608028654
GA = 0.044715


T3 = (0, 1, 2)
KB = tuple((k, b) for k in T3 for b in T3)
LANES = tuple(slice(k, k + 128) for k in range(0, C, 128))


def _mul(v, m):
    return pl.multiple_of(v, m)


def _rows(i, n):
    return pl.ds(_mul(i * n, n), n)


def _tiles(f):
    @pl.loop(0, TH)
    def _(i):
        for s in LANES:
            f(_rows(i, TW), s)


def _blocks(f):
    @pl.loop(0, 4)
    def _(i):
        f(i, _mul(i * 512, 512), _rows(i, 512))


def _load(pairs, sem):
    copies = [pltpu.make_async_copy(a, b, sem.at[i]) for i, (a, b) in enumerate(pairs)]
    for c in copies:
        c.start()
    return copies


def _gelu_parts(n):
    n2 = n * n
    t = jnp.tanh(GC * n * (1.0 + GA * n2))
    return n2, t


def _halo_scratch():
    return [pltpu.VMEM((16, C), BF), pltpu.VMEM((3, 16, C), BF), pltpu.VMEM((2, TW, C), BF), pltpu.VMEM((16, C), F32), pltpu.VMEM((10, 8, C), F32),
            pltpu.SemaphoreType.DMA((5,)), pltpu.SemaphoreType.DMA((5,))]


class _Halo:
    def __init__(self, src, scratch):
        self.src = src
        self.edge, self.cols, self.rows, self.colf, self.colp, self.ssem, self.rsem = scratch
        self.w, self.h = lax.axis_index('w'), lax.axis_index('h')

    def _copy(self, i, a, b, dev):
        return pltpu.make_async_remote_copy(src_ref=a, dst_ref=b, send_sem=self.ssem.at[i], recv_sem=self.rsem.at[i], device_id=dev, device_id_type=MESH)

    def _copies(self):
        w, h = self.w, self.h
        return (self._copy(0, self.edge, self.cols.at[1], (1 - w, h)),
                self._copy(1, self.edge, self.cols.at[0], (1 - w, h + 1)),
                self._copy(2, self.edge, self.cols.at[2], (1 - w, h - 1)),
                self._copy(3, self.src.at[pl.ds(PIX - TW, TW)], self.rows.at[0], (w, h + 1)),
                self._copy(4, self.src.at[pl.ds(0, TW)], self.rows.at[1], (w, h - 1)))

    def start(self, nh=8):
        w, h = self.w, self.h
        c = self._copies()

        @pl.when(h < nh - 1)
        def _():
            c[3].start()

        @pl.when(h > 0)
        def _():
            c[4].start()
        for i in range(TH):
            first = self.src[i * TW:i * TW + 16, :].astype(F32)[0:1]
            last = self.src[i * TW + TW - 16:i * TW + TW, :].astype(F32)[15:16]
            self.colf[i:i + 1, :] = jnp.where(w == 0, last, first)
        self.colf[8:16, :] = jnp.zeros((8, C), F32)
        self.edge[...] = self.colf[...].astype(BF)
        c[0].start()

        @pl.when(h < nh - 1)
        def _():
            c[1].start()

        @pl.when(h > 0)
        def _():
            c[2].start()

        @pl.when(h == 0)
        def _():
            self.rows[0] = jnp.zeros((TW, C), BF)
            self.cols[0] = jnp.zeros((16, C), BF)

        @pl.when(h == nh - 1)
        def _():
            self.rows[1] = jnp.zeros((TW, C), BF)
            self.cols[2] = jnp.zeros((16, C), BF)

    def wait_cols(self, nh=8):
        h = self.h
        c = self._copies()
        c[0].wait()

        @pl.when(h < nh - 1)
        def _():
            c[1].wait_send()
            c[2].wait_recv()

        @pl.when(h > 0)
        def _():
            c[2].wait_send()
            c[1].wait_recv()
        self.colp[0, 0:1, :] = self.cols[0].astype(F32)[7:8]
        mine = self.cols[1].astype(F32)
        for i in range(TH):
            self.colp[i + 1, 0:1, :] = mine[i:i + 1]
        self.colp[9, 0:1, :] = self.cols[2].astype(F32)[0:1]

    def wait_rows(self, nh=8):
        h = self.h
        c = self._copies()

        @pl.when(h < nh - 1)
        def _():
            c[3].wait_send()
            c[4].wait_recv()

        @pl.when(h > 0)
        def _():
            c[4].wait_send()
            c[3].wait_recv()

    def row(self, cat, r, load):
        w = self.w
        ids = lax.broadcasted_iota(jnp.int32, (TW, 128), 0)
        out = pl.ds(r * TW if isinstance(r, int) else pl.multiple_of(r * TW, TW), TW)
        for s in LANES:
            k = s.start
            x = load(s)
            xf = x.astype(F32)
            p = self.colp[r, 0:1, s]
            pl_ = jnp.where(w == 1, p, 0.0)
            pr = jnp.where(w == 0, p, 0.0)
            cat[out, s] = jnp.where(ids == 0, pl_, pltpu.roll(xf, 1, 0)).astype(BF)
            cat[out, C + k:C + k + 128] = x
            cat[out, 2 * C + k:2 * C + k + 128] = jnp.where(ids == TW - 1, pr, pltpu.roll(xf, TW - 1, 0)).astype(BF)

    def center(self, cat, r):
        o = pl.multiple_of((r - 1) * TW, TW)
        self.row(cat, r, lambda s: self.src[pl.ds(o, TW), s])

    def centers(self, cat):
        @pl.loop(1, TH + 1)
        def _(r):
            self.center(cat, r)

    def borders(self, cat):
        self.row(cat, 0, lambda s: self.rows[0, :, s])
        self.row(cat, TH + 1, lambda s: self.rows[1, :, s])


def _exchange(buf, ssem, rsem, nh=8, nw=2):
    w, h = lax.axis_index('w'), lax.axis_index('h')
    me = w * nh + h
    n = nh * nw
    copies = []
    for d in range(1, n):
        to = lax.rem(me + d, n)
        copies.append(pltpu.make_async_remote_copy(
            src_ref=buf.at[0], dst_ref=buf.at[d], send_sem=ssem.at[d], recv_sem=rsem.at[d],
            device_id=(to // nh, lax.rem(to, nh)), device_id_type=MESH))
    for c in copies:
        c.start()
    return copies


def _exchange_sum(buf, copies, nh=8, nw=2):
    w, h = lax.axis_index('w'), lax.axis_index('h')
    me = w * nh + h
    n = nh * nw
    for c in copies:
        c.wait()
    total = None
    for src in range(n):
        v = buf[lax.rem(me - src + n, n)]
        total = v if total is None else total + v
    return total


def _group_mats():
    cg = C // GROUPS
    ch = lax.broadcasted_iota(jnp.int32, (C, 128), 0)
    gr = lax.broadcasted_iota(jnp.int32, (C, 128), 1) * cg
    down = jnp.where((ch >= gr) & (ch < gr + cg), 1.0, 0.0).astype(F32)
    ch = lax.broadcasted_iota(jnp.int32, (128, C), 1)
    gr = lax.broadcasted_iota(jnp.int32, (128, C), 0) * cg
    up = jnp.where((ch >= gr) & (ch < gr + cg), 1.0, 0.0).astype(F32)
    return down, up


def _dotf(a, b):
    return jnp.dot(a, b, preferred_element_type=F32, precision=lax.Precision.HIGHEST)


def _conv(cat, w, m0, mb):
    acc = None
    for a in range(3):
        d = jnp.dot(cat[pl.ds(pl.multiple_of(m0 + a * TW, TW), mb), :], w[a], preferred_element_type=F32)
        acc = d if acc is None else acc + d
    return acc


def _conv_t(cat, w, m0, mb):
    acc = None
    for a in range(3):
        rows = pl.ds(pl.multiple_of(m0 + a * TW, TW), mb)
        for b in range(3):
            d = lax.dot_general(cat[rows, b * C:b * C + C], w[2 - a, (2 - b) * C:(2 - b) * C + C, :],
                                (((1,), (1,)), ((), ())), preferred_element_type=F32)
            acc = d if acc is None else acc + d
    return acc


def _k1(cnt, x, w1, g, gamma, beta, gcat_o, a_o, z_o, zt_o, xt_o, stat_o,
        xv, gv, wv, cat, gcat, av, zv, ztv, xtv, sums, ebuf, ess, ers, dsem, osem, *hs):
    n = len(hs) // 2
    hx, hg = _Halo(xv, hs[:n]), _Halo(gv, hs[n:])
    cx, cg, cw = _load(((x, xv), (g, gv), (w1, wv)), dsem)
    cx.wait()
    hx.start()
    cg.wait()
    hg.start()
    sums[...] = jnp.zeros_like(sums)
    hx.wait_cols()
    hx.centers(cat)
    hx.wait_rows()
    hx.borders(cat)
    hg.wait_cols()
    cw.wait()

    def conv(i, m0, m):
        a = _conv(cat, wv, m0, 512).astype(BF)
        av[m, :] = a
        af = a.astype(F32)
        sums[0:1, :] += jnp.sum(af, axis=0, keepdims=True)
        sums[1:2, :] += jnp.sum(af * af, axis=0, keepdims=True)
        for r in (2 * i, 2 * i + 1):
            hg.center(gcat, r + 1)
            for s in LANES:
                xtv[s, _rows(r, TW)] = xv[_rows(r, TW), s].astype(F32).T.astype(BF)
    _blocks(conv)
    down, up = _group_mats()
    ebuf[0] = _dotf(sums[...], down)
    copies = _exchange(ebuf, ess, ers)
    outs = _load(((av, a_o), (xtv, xt_o)), osem)
    hg.wait_rows()
    hg.borders(gcat)
    outs += _load(((gcat, gcat_o),), dsem)
    tot = _exchange_sum(ebuf, copies) * (1.0 / cnt)
    mean_g = tot[0:1]
    rstd_g = lax.rsqrt(tot[1:2] - mean_g * mean_g + EPS)
    row = lax.broadcasted_iota(jnp.int32, (8, 128), 0)
    st = jnp.where(row == 0, mean_g, jnp.where(row == 1, rstd_g, 0.0))
    st = _dotf(st, up)
    stat_o[...] = st
    sums[...] = st

    def act(m, s):
        nn = (av[m, s].astype(F32) - sums[0:1, s]) * sums[1:2, s] * gamma[:, s] + beta[:, s]
        _, t = _gelu_parts(nn)
        z = nn * (0.5 * (1.0 + t))
        zv[m, s] = z.astype(BF)
        ztv[s, m] = z.T.astype(BF)
    _tiles(act)
    outs += _load(((zv, z_o), (ztv, zt_o)), dsem.at[pl.ds(1, 2)])
    for c in outs:
        c.wait()


def _wgrad_block(lt, cat, a, c0):
    rows = pl.ds(pl.multiple_of(c0, 32), 160)
    return jnp.dot(lt[rows, :], cat[pl.ds(pl.multiple_of((2 - a) * TW, TW), PIX), :], preferred_element_type=F32)


class _Place:
    def __init__(self):
        self.w, self.h = lax.axis_index('w'), lax.axis_index('h')
        self.core = lax.rem(self.h, 2)
        self.chip = self.h // 2 + 4 * self.w

    def _axis(self, k):
        return 1 + k + k * (k - 1) // 2

    def bit(self, k):
        return lax.rem(self.chip // self._axis(k), 2)

    def across(self, k):
        chip = self.chip + self._axis(k) * (1 - 2 * self.bit(k))
        return chip // 4, lax.rem(chip, 4) * 2 + self.core

    def partner(self):
        return self.w, self.h + 1 - 2 * self.core


def _rcopy(src, dst, ss, rs, dev):
    return pltpu.make_async_remote_copy(src_ref=src, dst_ref=dst, send_sem=ss, recv_sem=rs, device_id=dev, device_id_type=MESH)


DMA = pltpu.SemaphoreType.DMA
Q, HALF, QUART, EIGHTH = 160, 480, 80, 40


def _rs_buffers():
    return [pltpu.VMEM((12 * HALF, C), F32), pltpu.VMEM((6, HALF, C), F32), pltpu.VMEM((3, HALF, C), F32)]


def _rs_scratch():
    return [pltpu.VMEM((3, 3, QUART, C), F32), pltpu.VMEM((3, 3, EIGHTH, C), F32)] + [DMA((6,))] * 2 + [DMA((3,))] * 2 + [DMA((3, 3))] * 4


class _Scatter:
    def __init__(self, place, bufs, own):
        self.pl = place
        self.p, self.d, self.r1 = bufs
        self.r2, self.r3, self.ds, self.dr, self.s1, self.q1, self.s2, self.q2, self.s3, self.q3 = own

    def _d2d(self, i):
        return _rcopy(self.p.at[_rows(i, HALF), :], self.d.at[i], self.ds.at[i], self.dr.at[i], self.pl.partner())

    def _rs1(self, k):
        return _rcopy(self.p.at[_rows(k + 6, HALF), :], self.r1.at[k], self.s1.at[k], self.q1.at[k], self.pl.across(k))

    def _half(self, k, d, n):
        return self.pl.bit((k + d) % 3) * n

    def _at(self, k, b, o, n):
        return pl.ds(_mul((k + 9) * HALF + b * Q + o, 8), n)

    def _rs2(self, k, b):
        src = self.p.at[self._at(k, b, QUART - self._half(k, 1, QUART), QUART), :]
        return _rcopy(src, self.r2.at[k, b], self.s2.at[k, b], self.q2.at[k, b], self.pl.across((k + 1) % 3))

    def _rs3(self, k, b):
        src = self.p.at[self._at(k, b, self._half(k, 1, QUART) + EIGHTH - self._half(k, 2, EIGHTH), EIGHTH), :]
        return _rcopy(src, self.r3.at[k, b], self.s3.at[k, b], self.q3.at[k, b], self.pl.across((k + 2) % 3))

    def block(self, j, lt, cat):
        me = self.pl
        phase, k = j // 3, lax.rem(j, 3)
        own, keep = lax.rem(phase, 2), phase // 2
        b1 = me.bit(k)
        core = me.core * own + (1 - me.core) * (1 - own)
        half = b1 * keep + (1 - b1) * (1 - keep)
        i = keep * 3 + k
        base = (own * 6 + i) * HALF
        acc = _wgrad_block(lt, cat, k, core * 2 * Q + half * Q)
        for b in T3:
            lo = (2 - b) * C
            self.p[pl.ds(_mul(base + b * Q, Q), Q), :] = acc[:, lo:lo + C]

        @pl.when(own == 0)
        def _():
            self._d2d(i).start()

        @pl.when(own == 1)
        def _():
            self._d2d(i).wait_recv()
            self.p[pl.ds(_mul(base, Q), HALF), :] += self.d[i]

        @pl.when(phase == 1)
        def _():
            self._rs1(k).start()

    def event1(self):
        for k in T3:
            self._rs1(k).wait_recv()
            s = self._half(k, 1, QUART)
            for o, go in ((QUART - s, True), (s, False)):
                for b in T3:
                    self.p[self._at(k, b, o, QUART), :] += self.r1[k, pl.ds(_mul(b * Q + o, 8), QUART), :]
                    if go:
                        self._rs2(k, b).start()

    def event2(self):
        for k in T3:
            s, t = self._half(k, 1, QUART), self._half(k, 2, EIGHTH)
            for b in T3:
                self._rs2(k, b).wait_recv()
            for o, go in ((EIGHTH - t, True), (t, False)):
                for b in T3:
                    self.p[self._at(k, b, s + o, EIGHTH), :] += self.r2[k, b, pl.ds(_mul(o, 8), EIGHTH), :]
                    if go:
                        self._rs3(k, b).start()

    def event3(self, f):
        for k, b in KB:
            self._rs3(k, b).wait_recv()
            f[k, b] = self.p[self._at(k, b, self._half(k, 1, QUART) + self._half(k, 2, EIGHTH), EIGHTH), :] + self.r3[k, b]

    def sent(self):
        for i in range(6):
            self._d2d(i).wait_send()

    def finish(self):
        for k in T3:
            self._rs1(k).wait_send()
        for k, b in KB:
            self._rs2(k, b).wait_send()
            self._rs3(k, b).wait_send()


def _ag_scratch():
    return [DMA((3,))] * 7 + [DMA((3, 3))] * 4


class _Gather:
    def __init__(self, place, f, out, sems):
        self.pl, self.f, self.out = place, f, out
        self.loc, self.s1, self.r1, self.s2, self.r2, self.fas, self.far, self.s3, self.r3, self.fbs, self.fbr = sems

    def _rows(self, k, depth):
        o, n = self.pl.core * 2 * Q, 2 * Q
        for d in range(depth):
            n = n // 2
            o = o + self.pl.bit((k + d) % 3) * n
        return pl.ds(_mul(o, 8), n)

    def _at(self, k, depth):
        return self.out.at[k, :, self._rows(k, depth), :]

    def _local(self, k):
        return pltpu.make_async_copy(self.f.at[k], self._at(k, 3), self.loc.at[k])

    def _c1(self, k):
        return _rcopy(self.f.at[k], self._at(k, 3), self.s1.at[k], self.r1.at[k], self.pl.across((k + 2) % 3))

    def _c2(self, k):
        r = self._at(k, 2)
        return _rcopy(r, r, self.s2.at[k], self.r2.at[k], self.pl.across((k + 1) % 3))

    def _c3(self, k, b):
        r = self.out.at[k, b, self._rows(k, 1), :]
        return _rcopy(r, r, self.s3.at[k, b], self.r3.at[k, b], self.pl.across(k))

    def _fa(self, k):
        r = self._at(k, 1)
        return _rcopy(r, r, self.fas.at[k], self.far.at[k], self.pl.partner())

    def _fb(self, k, b):
        o = self.pl.core * 2 * Q + (1 - self.pl.bit(k)) * Q
        r = self.out.at[k, b, pl.ds(_mul(o, 8), Q), :]
        return _rcopy(r, r, self.fbs.at[k, b], self.fbr.at[k, b], self.pl.partner())

    def start(self):
        for k in T3:
            self._c1(k).start()
            self._local(k).start()

    def event1(self):
        for k in T3:
            self._local(k).wait()
            self._c1(k).wait_recv()
            self._c2(k).start()

    def event2(self):
        for k in T3:
            self._c2(k).wait_recv()
            for b in T3:
                self._c3(k, b).start()
            self._fa(k).start()

    def event3(self):
        for b in T3:
            for k in T3:
                self._c3(k, b).wait_recv()
                self._fb(k, b).start()

    def finish(self):
        for k in T3:
            self._c1(k).wait_send()
            self._c2(k).wait_send()
            self._fa(k).wait()
        for k, b in KB:
            self._c3(k, b).wait_send()
            self._fb(k, b).wait()


def _k2(cnt, gcat_i, zt_i, a_i, stat, gamma, beta, w2, w1, xt, x, z, g, dw1_o, dw2_o, y_o, dx_o, t_o,
        cat, lt, av, wv, zv, sums, ebuf, ess, ers, dsem, esem, f1, f2, *sc):
    sc = list(sc)

    def take(group):
        n = len(group)
        out, sc[:n] = sc[:n], []
        return out
    place = _Place()
    hd, hz = _Halo(av, take(_halo_scratch())), _Halo(zv, take(_halo_scratch()))
    bufs = take(_rs_buffers())
    rs2, rs1 = _Scatter(place, bufs, take(_rs_scratch())), _Scatter(place, bufs, take(_rs_scratch()))
    ag2, ag1 = _Gather(place, f2, dw2_o, take(_ag_scratch())), _Gather(place, f1, dw1_o, take(_ag_scratch()))
    dn = bufs[0]
    ins = _load(((zt_i, lt), (gcat_i, cat), (w2, wv), (a_i, av), (z, zv)), dsem)
    sums[...] = jnp.zeros_like(sums)
    ins[0].wait()
    ins[1].wait()

    @pl.loop(0, 12)
    def _(j):
        rs2.block(j, lt, cat)
    for c in ins[2:]:
        c.wait()
    cxt, = _load(((xt, lt),), esem)
    hz.start()
    rs2.sent()

    def dz_block(i, m0, m):
        dn[m, :] = _conv_t(cat, wv, m0, 512)
        for q in (2 * i, 2 * i + 1):
            for s in LANES:
                mm = _rows(q, TW)
                xh = (av[mm, s].astype(F32) - stat[0:1, s]) * stat[1:2, s]
                nn = xh * gamma[:, s] + beta[:, s]
                n2, t = _gelu_parts(nn)
                d = dn[mm, s] * (0.5 * (1.0 + t) + (0.5 * GC) * nn * (1.0 - t * t) * (1.0 + (3.0 * GA) * n2))
                dn[mm, s] = d
                sums[0:1, s] += jnp.sum(d * xh, axis=0, keepdims=True)
                sums[1:2, s] += jnp.sum(d, axis=0, keepdims=True)

        @pl.when(i == 2)
        def _():
            rs2.event1()
    _blocks(dz_block)
    cw1, = _load(((w1, wv),), dsem)
    ebuf[0] = jnp.zeros((16, 128), F32)
    for k, l in enumerate(LANES):
        for s in (0, 1):
            ebuf[0, s * 8 + k:s * 8 + k + 1, :] = sums[s:s + 1, l]
    tot = _exchange_sum(ebuf, _exchange(ebuf, ess, ers))
    for k, l in enumerate(LANES):
        for s in (0, 1):
            sums[s:s + 1, l] = tot[s * 8 + k:s * 8 + k + 1, :]
    t_o[...] = sums[...]
    down, up = _group_mats()
    sums[...] = _dotf(_dotf(sums[...] * gamma[...], down) * (1.0 / cnt), up)

    def da_tile(m, s):
        xh = (av[m, s].astype(F32) - stat[0:1, s]) * stat[1:2, s]
        av[m, s] = (stat[1:2, s] * (dn[m, s] * gamma[:, s] - sums[1:2, s] - xh * sums[0:1, s])).astype(BF)
    _tiles(da_tile)
    hd.start()
    rs2.event2()
    hd.wait_cols()
    hd.centers(cat)
    hd.wait_rows()
    hd.borders(cat)
    cgv, = _load(((g, av),), dsem.at[pl.ds(1, 1)])
    rs2.event3(f2)
    ag2.start()
    rs2.finish()
    cxt.wait()

    @pl.loop(0, 12)
    def _(j):
        rs1.block(j, lt, cat)

        @pl.when(j == 4)
        def _():
            ag2.event1()
    cw1.wait()
    cgv.wait()

    def dx_block(i, m0, m):
        av[m, :] = (_conv_t(cat, wv, m0, 512) + av[m, :].astype(F32)).astype(BF)

        @pl.when(i == 2)
        def _():
            rs1.event1()
            ag2.event2()
    _blocks(dx_block)
    cdx, cw2 = _load(((av, dx_o), (w2, wv)), dsem)
    hz.wait_cols()
    hz.centers(cat)
    hz.wait_rows()
    hz.borders(cat)
    cxv, = _load(((x, zv),), esem)
    rs1.event2()
    cw2.wait()
    cxv.wait()

    def y_block(i, m0, m):
        zv[m, :] = (_conv(cat, wv, m0, 512) + zv[m, :].astype(F32)).astype(BF)

        @pl.when(i == 2)
        def _():
            rs1.event3(f1)
            ag1.start()
    _blocks(y_block)
    cy, = _load(((zv, y_o),), esem)
    ag1.event1()
    ag2.event3()
    ag1.event2()
    cdx.wait()
    cy.wait()
    rs1.sent()
    rs1.finish()
    ag2.finish()
    ag1.event3()
    ag1.finish()


def _params(**kw):
    return pltpu.CompilerParams(has_side_effects=True, vmem_limit_bytes=64 * 2**20 - 65536, **kw)


def solution(mesh):
    tile = P(None, 'h', 'w', None)
    cnt = float(TH * TW * 16 * (C // GROUPS))
    sds = jax.ShapeDtypeStruct
    V = pltpu.VMEM

    def body(x, w1, gamma, beta, w2, g):
        x2, g2 = x.reshape(PIX, C), g.reshape(PIX, C)
        w1r, w2r = w1.reshape(3, 3 * C, C), w2.reshape(3, 3 * C, C)
        ga, be = gamma.reshape(1, C), beta.reshape(1, C)
        tile, flip, wide, wts = sds((PIX, C), BF), sds((C, PIX), BF), sds((10 * TW, 3 * C), BF), sds((3, 3 * C, C), BF)
        dw = sds((3, 3, C, C), F32)
        vm = lambda l: [V(a.shape, a.dtype) for a in l]
        sums = [V((8, C), F32)]
        sems = [DMA((16,)), DMA((16,)), DMA((8,)), DMA((2,))]
        gcat, a, z, zt, xt, stat = pl.pallas_call(
            lambda *r: _k1(cnt, *r),
            out_shape=[wide, tile, tile, flip, flip, sds((8, C), F32)],
            in_specs=[ANY] * 3 + [VM] * 2, out_specs=[ANY] * 5 + [VM],
            scratch_shapes=vm((tile, tile, wts, wide, wide, tile, tile, flip, flip)) + sums + [V((16, 8, 128), F32)] + sems + _halo_scratch() * 2,
            compiler_params=_params(), name='k1')(x2, w1r, g2, ga, be)
        dw1, dw2, y, dx, t = pl.pallas_call(
            lambda *r: _k2(cnt, *r),
            out_shape=[dw, dw, tile, tile, sds((8, C), F32)],
            in_specs=[ANY] * 3 + [VM] * 3 + [ANY] * 6, out_specs=[ANY] * 4 + [VM],
            scratch_shapes=vm((wide, flip, tile, wts, tile)) + sums + [V((16, 16, 128), F32)] + sems + [V((3, 3, EIGHTH, C), F32)] * 2
            + _halo_scratch() * 2 + _rs_buffers() + _rs_scratch() * 2 + _ag_scratch() * 2,
            compiler_params=_params(), name='k2')(gcat, zt, a, stat, ga, be, w2r, w1r, xt, x2, z, g2)
        return y.reshape(x.shape), dx.reshape(x.shape), dw1, dw2, t[0], t[1]

    return jax.shard_map(body, mesh=mesh, in_specs=(tile, P(), P(), P(), P(), tile), out_specs=(tile, tile, P(), P(), P(), P()), check_vma=False)
```

```python
import jax
import jax.numpy as jnp
from jax import lax
from jax.experimental import pallas as pl
from jax.experimental.pallas import tpu as pltpu
from jax.sharding import PartitionSpec as P

GROUPS = 32
EPS = 1e-5
MESH = pl.DeviceIdType.MESH
F32 = jnp.float32
BF = jnp.bfloat16
ANY = pl.BlockSpec(memory_space=pl.ANY)
VM = pl.BlockSpec(memory_space=pltpu.VMEM)
TH, TW, C = 8, 256, 640
PIX = TH * TW
GC = 0.7978845608028654
GA = 0.044715


T3 = (0, 1, 2)
KB = tuple((k, b) for k in T3 for b in T3)
LANES = tuple(slice(k, k + 128) for k in range(0, C, 128))


def _mul(v, m):
    return pl.multiple_of(v, m)


def _rows(i, n):
    return pl.ds(_mul(i * n, n), n)


def _tiles(f):
    @pl.loop(0, TH)
    def _(i):
        for s in LANES:
            f(_rows(i, TW), s)


def _blocks(f):
    @pl.loop(0, 4)
    def _(i):
        f(i, _mul(i * 512, 512), _rows(i, 512))


def _load(pairs, sem):
    copies = [pltpu.make_async_copy(a, b, sem.at[i]) for i, (a, b) in enumerate(pairs)]
    for c in copies:
        c.start()
    return copies


def _gelu_parts(n):
    n2 = n * n
    t = jnp.tanh(GC * n * (1.0 + GA * n2))
    return n2, t


def _halo_scratch():
    return [pltpu.VMEM((16, C), BF), pltpu.VMEM((3, 16, C), BF), pltpu.VMEM((2, TW, C), BF), pltpu.VMEM((16, C), F32), pltpu.VMEM((10, 8, C), F32),
            pltpu.SemaphoreType.DMA((5,)), pltpu.SemaphoreType.DMA((5,))]


class _Halo:
    def __init__(self, src, scratch):
        self.src = src
        self.edge, self.cols, self.rows, self.colf, self.colp, self.ssem, self.rsem = scratch
        self.w, self.h = lax.axis_index('w'), lax.axis_index('h')

    def _copy(self, i, a, b, dev):
        return pltpu.make_async_remote_copy(src_ref=a, dst_ref=b, send_sem=self.ssem.at[i], recv_sem=self.rsem.at[i], device_id=dev, device_id_type=MESH)

    def _copies(self):
        w, h = self.w, self.h
        return (self._copy(0, self.edge, self.cols.at[1], (1 - w, h)),
                self._copy(1, self.edge, self.cols.at[0], (1 - w, h + 1)),
                self._copy(2, self.edge, self.cols.at[2], (1 - w, h - 1)),
                self._copy(3, self.src.at[pl.ds(PIX - TW, TW)], self.rows.at[0], (w, h + 1)),
                self._copy(4, self.src.at[pl.ds(0, TW)], self.rows.at[1], (w, h - 1)))

    def start(self, nh=8):
        w, h = self.w, self.h
        c = self._copies()

        @pl.when(h < nh - 1)
        def _():
            c[3].start()

        @pl.when(h > 0)
        def _():
            c[4].start()
        for i in range(TH):
            first = self.src[i * TW:i * TW + 16, :].astype(F32)[0:1]
            last = self.src[i * TW + TW - 16:i * TW + TW, :].astype(F32)[15:16]
            self.colf[i:i + 1, :] = jnp.where(w == 0, last, first)
        self.colf[8:16, :] = jnp.zeros((8, C), F32)
        self.edge[...] = self.colf[...].astype(BF)
        c[0].start()

        @pl.when(h < nh - 1)
        def _():
            c[1].start()

        @pl.when(h > 0)
        def _():
            c[2].start()

        @pl.when(h == 0)
        def _():
            self.rows[0] = jnp.zeros((TW, C), BF)
            self.cols[0] = jnp.zeros((16, C), BF)

        @pl.when(h == nh - 1)
        def _():
            self.rows[1] = jnp.zeros((TW, C), BF)
            self.cols[2] = jnp.zeros((16, C), BF)

    def wait_cols(self, nh=8):
        h = self.h
        c = self._copies()
        c[0].wait()

        @pl.when(h < nh - 1)
        def _():
            c[1].wait_send()
            c[2].wait_recv()

        @pl.when(h > 0)
        def _():
            c[2].wait_send()
            c[1].wait_recv()
        self.colp[0, 0:1, :] = self.cols[0].astype(F32)[7:8]
        mine = self.cols[1].astype(F32)
        for i in range(TH):
            self.colp[i + 1, 0:1, :] = mine[i:i + 1]
        self.colp[9, 0:1, :] = self.cols[2].astype(F32)[0:1]

    def wait_rows(self, nh=8):
        h = self.h
        c = self._copies()

        @pl.when(h < nh - 1)
        def _():
            c[3].wait_send()
            c[4].wait_recv()

        @pl.when(h > 0)
        def _():
            c[4].wait_send()
            c[3].wait_recv()

    def row(self, cat, r, load):
        w = self.w
        ids = lax.broadcasted_iota(jnp.int32, (TW, 128), 0)
        out = pl.ds(r * TW if isinstance(r, int) else pl.multiple_of(r * TW, TW), TW)
        for s in LANES:
            k = s.start
            x = load(s)
            xf = x.astype(F32)
            p = self.colp[r, 0:1, s]
            pl_ = jnp.where(w == 1, p, 0.0)
            pr = jnp.where(w == 0, p, 0.0)
            cat[out, s] = jnp.where(ids == 0, pl_, pltpu.roll(xf, 1, 0)).astype(BF)
            cat[out, C + k:C + k + 128] = x
            cat[out, 2 * C + k:2 * C + k + 128] = jnp.where(ids == TW - 1, pr, pltpu.roll(xf, TW - 1, 0)).astype(BF)

    def center(self, cat, r):
        o = pl.multiple_of((r - 1) * TW, TW)
        self.row(cat, r, lambda s: self.src[pl.ds(o, TW), s])

    def centers(self, cat):
        @pl.loop(1, TH + 1)
        def _(r):
            self.center(cat, r)

    def borders(self, cat):
        self.row(cat, 0, lambda s: self.rows[0, :, s])
        self.row(cat, TH + 1, lambda s: self.rows[1, :, s])


def _exchange(buf, ssem, rsem, nh=8, nw=2):
    w, h = lax.axis_index('w'), lax.axis_index('h')
    me = w * nh + h
    n = nh * nw
    copies = []
    for d in range(1, n):
        to = lax.rem(me + d, n)
        copies.append(pltpu.make_async_remote_copy(
            src_ref=buf.at[0], dst_ref=buf.at[d], send_sem=ssem.at[d], recv_sem=rsem.at[d],
            device_id=(to // nh, lax.rem(to, nh)), device_id_type=MESH))
    for c in copies:
        c.start()
    return copies


def _exchange_sum(buf, copies, nh=8, nw=2):
    w, h = lax.axis_index('w'), lax.axis_index('h')
    me = w * nh + h
    n = nh * nw
    for c in copies:
        c.wait()
    total = None
    for src in range(n):
        v = buf[lax.rem(me - src + n, n)]
        total = v if total is None else total + v
    return total


def _group_mats():
    cg = C // GROUPS
    ch = lax.broadcasted_iota(jnp.int32, (C, 128), 0)
    gr = lax.broadcasted_iota(jnp.int32, (C, 128), 1) * cg
    down = jnp.where((ch >= gr) & (ch < gr + cg), 1.0, 0.0).astype(F32)
    ch = lax.broadcasted_iota(jnp.int32, (128, C), 1)
    gr = lax.broadcasted_iota(jnp.int32, (128, C), 0) * cg
    up = jnp.where((ch >= gr) & (ch < gr + cg), 1.0, 0.0).astype(F32)
    return down, up


def _dotf(a, b):
    return jnp.dot(a, b, preferred_element_type=F32, precision=lax.Precision.HIGHEST)


def _conv(cat, w, m0, mb):
    acc = None
    for a in range(3):
        d = jnp.dot(cat[pl.ds(pl.multiple_of(m0 + a * TW, TW), mb), :], w[a], preferred_element_type=F32)
        acc = d if acc is None else acc + d
    return acc


def _conv_t(cat, w, m0, mb):
    acc = None
    for a in range(3):
        rows = pl.ds(pl.multiple_of(m0 + a * TW, TW), mb)
        for b in range(3):
            d = lax.dot_general(cat[rows, b * C:b * C + C], w[2 - a, (2 - b) * C:(2 - b) * C + C, :],
                                (((1,), (1,)), ((), ())), preferred_element_type=F32)
            acc = d if acc is None else acc + d
    return acc


def _k1(cnt, x, w1, g, gamma, beta, gcat_o, a_o, z_o, zt_o, xt_o, stat_o,
        xv, gv, wv, cat, gcat, av, zv, ztv, xtv, sums, ebuf, ess, ers, dsem, osem, *hs):
    n = len(hs) // 2
    hx, hg = _Halo(xv, hs[:n]), _Halo(gv, hs[n:])
    cx, cg, cw = _load(((x, xv), (g, gv), (w1, wv)), dsem)
    cx.wait()
    hx.start()
    cg.wait()
    hg.start()
    sums[...] = jnp.zeros_like(sums)
    hx.wait_cols()
    hx.centers(cat)
    hx.wait_rows()
    hx.borders(cat)
    hg.wait_cols()
    cw.wait()

    def conv(i, m0, m):
        a = _conv(cat, wv, m0, 512).astype(BF)
        av[m, :] = a
        af = a.astype(F32)
        sums[0:1, :] += jnp.sum(af, axis=0, keepdims=True)
        sums[1:2, :] += jnp.sum(af * af, axis=0, keepdims=True)
        for r in (2 * i, 2 * i + 1):
            hg.center(gcat, r + 1)
            for s in LANES:
                xtv[s, _rows(r, TW)] = xv[_rows(r, TW), s].astype(F32).T.astype(BF)
    _blocks(conv)
    down, up = _group_mats()
    ebuf[0] = _dotf(sums[...], down)
    copies = _exchange(ebuf, ess, ers)
    outs = _load(((av, a_o), (xtv, xt_o)), osem)
    hg.wait_rows()
    hg.borders(gcat)
    outs += _load(((gcat, gcat_o),), dsem)
    tot = _exchange_sum(ebuf, copies) * (1.0 / cnt)
    mean_g = tot[0:1]
    rstd_g = lax.rsqrt(tot[1:2] - mean_g * mean_g + EPS)
    row = lax.broadcasted_iota(jnp.int32, (8, 128), 0)
    st = jnp.where(row == 0, mean_g, jnp.where(row == 1, rstd_g, 0.0))
    st = _dotf(st, up)
    stat_o[...] = st
    sums[...] = st

    def act(m, s):
        nn = (av[m, s].astype(F32) - sums[0:1, s]) * sums[1:2, s] * gamma[:, s] + beta[:, s]
        _, t = _gelu_parts(nn)
        z = nn * (0.5 * (1.0 + t))
        zv[m, s] = z.astype(BF)
        ztv[s, m] = z.T.astype(BF)
    _tiles(act)
    outs += _load(((zv, z_o), (ztv, zt_o)), dsem.at[pl.ds(1, 2)])
    for c in outs:
        c.wait()


def _wgrad_block(lt, cat, a, c0):
    rows = pl.ds(pl.multiple_of(c0, 32), 160)
    return jnp.dot(lt[rows, :], cat[pl.ds(pl.multiple_of((2 - a) * TW, TW), PIX), :], preferred_element_type=F32)


class _Place:
    def __init__(self):
        self.w, self.h = lax.axis_index('w'), lax.axis_index('h')
        self.core = lax.rem(self.h, 2)
        self.chip = self.h // 2 + 4 * self.w

    def _axis(self, k):
        return 1 + k + k * (k - 1) // 2

    def bit(self, k):
        return lax.rem(self.chip // self._axis(k), 2)

    def across(self, k):
        chip = self.chip + self._axis(k) * (1 - 2 * self.bit(k))
        return chip // 4, lax.rem(chip, 4) * 2 + self.core

    def partner(self):
        return self.w, self.h + 1 - 2 * self.core


def _rcopy(src, dst, ss, rs, dev):
    return pltpu.make_async_remote_copy(src_ref=src, dst_ref=dst, send_sem=ss, recv_sem=rs, device_id=dev, device_id_type=MESH)


DMA = pltpu.SemaphoreType.DMA
Q, HALF, QUART, EIGHTH = 160, 480, 80, 40


def _rs_buffers():
    return [pltpu.VMEM((12 * HALF, C), F32), pltpu.VMEM((6, HALF, C), F32), pltpu.VMEM((3, HALF, C), F32)]


def _rs_scratch():
    return [pltpu.VMEM((3, 3, QUART, C), F32), pltpu.VMEM((3, 3, EIGHTH, C), F32)] + [DMA((6,))] * 2 + [DMA((3,))] * 2 + [DMA((3, 3))] * 4


class _Scatter:
    def __init__(self, place, bufs, own):
        self.pl = place
        self.p, self.d, self.r1 = bufs
        self.r2, self.r3, self.ds, self.dr, self.s1, self.q1, self.s2, self.q2, self.s3, self.q3 = own

    def _d2d(self, i):
        return _rcopy(self.p.at[_rows(i, HALF), :], self.d.at[i], self.ds.at[i], self.dr.at[i], self.pl.partner())

    def _rs1(self, k):
        return _rcopy(self.p.at[_rows(k + 6, HALF), :], self.r1.at[k], self.s1.at[k], self.q1.at[k], self.pl.across(k))

    def _half(self, k, d, n):
        return self.pl.bit((k + d) % 3) * n

    def _at(self, k, b, o, n):
        return pl.ds(_mul((k + 9) * HALF + b * Q + o, 8), n)

    def _rs2(self, k, b):
        src = self.p.at[self._at(k, b, QUART - self._half(k, 1, QUART), QUART), :]
        return _rcopy(src, self.r2.at[k, b], self.s2.at[k, b], self.q2.at[k, b], self.pl.across((k + 1) % 3))

    def _rs3(self, k, b):
        src = self.p.at[self._at(k, b, self._half(k, 1, QUART) + EIGHTH - self._half(k, 2, EIGHTH), EIGHTH), :]
        return _rcopy(src, self.r3.at[k, b], self.s3.at[k, b], self.q3.at[k, b], self.pl.across((k + 2) % 3))

    def block(self, j, lt, cat):
        me = self.pl
        phase, k = j // 3, lax.rem(j, 3)
        own, keep = lax.rem(phase, 2), phase // 2
        b1 = me.bit(k)
        core = me.core * own + (1 - me.core) * (1 - own)
        half = b1 * keep + (1 - b1) * (1 - keep)
        i = keep * 3 + k
        base = (own * 6 + i) * HALF
        acc = _wgrad_block(lt, cat, k, core * 2 * Q + half * Q)
        for b in T3:
            lo = (2 - b) * C
            self.p[pl.ds(_mul(base + b * Q, Q), Q), :] = acc[:, lo:lo + C]

        @pl.when(own == 0)
        def _():
            self._d2d(i).start()

        @pl.when(own == 1)
        def _():
            self._d2d(i).wait_recv()
            self.p[pl.ds(_mul(base, Q), HALF), :] += self.d[i]

        @pl.when(phase == 1)
        def _():
            self._rs1(k).start()

    def event1(self):
        for k in T3:
            self._rs1(k).wait_recv()
            s = self._half(k, 1, QUART)
            for o, go in ((QUART - s, True), (s, False)):
                for b in T3:
                    self.p[self._at(k, b, o, QUART), :] += self.r1[k, pl.ds(_mul(b * Q + o, 8), QUART), :]
                    if go:
                        self._rs2(k, b).start()

    def event2(self):
        for k in T3:
            s, t = self._half(k, 1, QUART), self._half(k, 2, EIGHTH)
            for b in T3:
                self._rs2(k, b).wait_recv()
            for o, go in ((EIGHTH - t, True), (t, False)):
                for b in T3:
                    self.p[self._at(k, b, s + o, EIGHTH), :] += self.r2[k, b, pl.ds(_mul(o, 8), EIGHTH), :]
                    if go:
                        self._rs3(k, b).start()

    def event3(self, f):
        for k, b in KB:
            self._rs3(k, b).wait_recv()
            f[k, b] = self.p[self._at(k, b, self._half(k, 1, QUART) + self._half(k, 2, EIGHTH), EIGHTH), :] + self.r3[k, b]

    def sent(self):
        for i in range(6):
            self._d2d(i).wait_send()

    def sent1(self):
        for k in T3:
            self._rs1(k).wait_send()

    def finish(self):
        for k, b in KB:
            self._rs2(k, b).wait_send()
            self._rs3(k, b).wait_send()


def _ag_scratch():
    return [DMA((3,))] * 7 + [DMA((3, 3))] * 4


class _Gather:
    def __init__(self, place, f, out, sems, vmem=False):
        self.pl, self.f, self.out, self.vmem = place, f, out, vmem
        self.loc, self.s1, self.r1, self.s2, self.r2, self.fas, self.far, self.s3, self.r3, self.fbs, self.fbr = sems

    def _rows(self, k, depth):
        o, n = self.pl.core * 2 * Q, 2 * Q
        for d in range(depth):
            n = n // 2
            o = o + self.pl.bit((k + d) % 3) * n
        return pl.ds(_mul(o, 8), n)

    def _at(self, k, depth):
        return self.out.at[k, :, self._rows(k, depth), :]

    def _local(self, k):
        return pltpu.make_async_copy(self.f.at[k], self._at(k, 3), self.loc.at[k])

    def _local_start(self, k):
        if self.vmem:
            self.out[k, :, self._rows(k, 3), :] = self.f[k]
        else:
            self._local(k).start()

    def _c1(self, k):
        return _rcopy(self.f.at[k], self._at(k, 3), self.s1.at[k], self.r1.at[k], self.pl.across((k + 2) % 3))

    def _c2(self, k):
        r = self._at(k, 2)
        return _rcopy(r, r, self.s2.at[k], self.r2.at[k], self.pl.across((k + 1) % 3))

    def _c3(self, k, b):
        r = self.out.at[k, b, self._rows(k, 1), :]
        return _rcopy(r, r, self.s3.at[k, b], self.r3.at[k, b], self.pl.across(k))

    def _fa(self, k):
        r = self._at(k, 1)
        return _rcopy(r, r, self.fas.at[k], self.far.at[k], self.pl.partner())

    def _fb(self, k, b):
        o = self.pl.core * 2 * Q + (1 - self.pl.bit(k)) * Q
        r = self.out.at[k, b, pl.ds(_mul(o, 8), Q), :]
        return _rcopy(r, r, self.fbs.at[k, b], self.fbr.at[k, b], self.pl.partner())

    def start(self):
        for k in T3:
            self._c1(k).start()
            self._local_start(k)

    def event1(self):
        for k in T3:
            if not self.vmem:
                self._local(k).wait()
            self._c1(k).wait_recv()
            self._c2(k).start()

    def event2(self, part=T3):
        for k in T3:
            if 0 in part:
                self._c2(k).wait_recv()
            for b in part:
                self._c3(k, b).start()
            if 0 in part:
                self._fa(k).start()

    def event3(self):
        for b in T3:
            for k in T3:
                self._c3(k, b).wait_recv()
                self._fb(k, b).start()

    def finish(self):
        for k in T3:
            self._c1(k).wait_send()
            self._c2(k).wait_send()
            self._fa(k).wait()
        for k, b in KB:
            self._c3(k, b).wait_send()
            self._fb(k, b).wait()


def _k2(cnt, gcat_i, zt_i, a_i, stat, gamma, beta, w2, w1, xt, x, z, g, dw2_o, y_o, dx_o, f1, t_o,
        cat, lt, av, wv, zv, sums, ebuf, ess, ers, dsem, esem, f2, *sc):
    sc = list(sc)

    def take(group):
        n = len(group)
        out, sc[:n] = sc[:n], []
        return out
    place = _Place()
    hd, hz = _Halo(av, take(_halo_scratch())), _Halo(zv, take(_halo_scratch()))
    bufs = take(_rs_buffers())
    rs2, rs1 = _Scatter(place, bufs, take(_rs_scratch())), _Scatter(place, bufs, take(_rs_scratch()))
    ag2 = _Gather(place, f2, dw2_o, take(_ag_scratch()))
    dn = bufs[0]
    ins = _load(((zt_i, lt), (gcat_i, cat), (w2, wv), (a_i, av), (z, zv)), dsem)
    sums[...] = jnp.zeros_like(sums)
    ins[0].wait()
    ins[1].wait()

    @pl.loop(0, 12)
    def _(j):
        rs2.block(j, lt, cat)
    for c in ins[2:]:
        c.wait()
    cxt, = _load(((xt, lt),), esem)
    hz.start()
    rs2.sent()

    def dz_block(i, m0, m):
        dn[m, :] = _conv_t(cat, wv, m0, 512)
        for q in (2 * i, 2 * i + 1):
            for s in LANES:
                mm = _rows(q, TW)
                xh = (av[mm, s].astype(F32) - stat[0:1, s]) * stat[1:2, s]
                nn = xh * gamma[:, s] + beta[:, s]
                n2, t = _gelu_parts(nn)
                d = dn[mm, s] * (0.5 * (1.0 + t) + (0.5 * GC) * nn * (1.0 - t * t) * (1.0 + (3.0 * GA) * n2))
                dn[mm, s] = d
                sums[0:1, s] += jnp.sum(d * xh, axis=0, keepdims=True)
                sums[1:2, s] += jnp.sum(d, axis=0, keepdims=True)

        @pl.when(i == 2)
        def _():
            rs2.event1()
    _blocks(dz_block)
    cw1, = _load(((w1, wv),), dsem)
    ebuf[0] = jnp.zeros((16, 128), F32)
    for k, l in enumerate(LANES):
        for s in (0, 1):
            ebuf[0, s * 8 + k:s * 8 + k + 1, :] = sums[s:s + 1, l]
    tot = _exchange_sum(ebuf, _exchange(ebuf, ess, ers))
    for k, l in enumerate(LANES):
        for s in (0, 1):
            sums[s:s + 1, l] = tot[s * 8 + k:s * 8 + k + 1, :]
    t_o[...] = sums[...]
    down, up = _group_mats()
    sums[...] = _dotf(_dotf(sums[...] * gamma[...], down) * (1.0 / cnt), up)

    def da_tile(m, s):
        xh = (av[m, s].astype(F32) - stat[0:1, s]) * stat[1:2, s]
        av[m, s] = (stat[1:2, s] * (dn[m, s] * gamma[:, s] - sums[1:2, s] - xh * sums[0:1, s])).astype(BF)
    _tiles(da_tile)
    hd.start()
    rs2.event2()
    hd.wait_cols()
    hd.centers(cat)
    hd.wait_rows()
    hd.borders(cat)
    cgv, = _load(((g, av),), dsem.at[pl.ds(1, 1)])
    rs2.sent1()
    cxt.wait()

    @pl.loop(0, 12)
    def _(j):
        rs1.block(j, lt, cat)

        @pl.when(j == 2)
        def _():
            rs2.event3(f2)
            ag2.start()

        @pl.when(j == 7)
        def _():
            ag2.event1()
            rs2.finish()
    cw1.wait()
    cgv.wait()

    def dx_block(i, m0, m):
        av[m, :] = (_conv_t(cat, wv, m0, 512) + av[m, :].astype(F32)).astype(BF)

        @pl.when(i == 3)
        def _():
            rs1.event1()
    _blocks(dx_block)
    cdx, cw2 = _load(((av, dx_o), (w2, wv)), dsem)
    hz.wait_cols()
    hz.centers(cat)
    hz.wait_rows()
    hz.borders(cat)
    cxv, = _load(((x, zv),), esem)
    cw2.wait()
    cxv.wait()

    def y_block(i, m0, m):
        zv[m, :] = (_conv(cat, wv, m0, 512) + zv[m, :].astype(F32)).astype(BF)

        @pl.when(i == 1)
        def _():
            ag2.event2((0,))

        @pl.when(i == 3)
        def _():
            rs1.event2()
            ag2.event2((1, 2))
    _blocks(y_block)
    cy, = _load(((zv, y_o),), esem)
    rs1.event3(f1)
    ag2.event3()
    cdx.wait()
    cy.wait()
    rs1.sent()
    rs1.sent1()
    rs1.finish()
    ag2.finish()


def _k3(f1, dw1_o, *sems):
    ag1 = _Gather(_Place(), f1, dw1_o, sems, True)
    ag1.start()
    ag1.event1()
    ag1.event2()
    ag1.event3()
    ag1.finish()


def _k4(dw1, dw2, y, dx, dw1_o, dw2_o, y_o, dx_o, dsem):
    for c in _load(((dw1, dw1_o), (dw2, dw2_o), (y, y_o), (dx, dx_o)), dsem):
        c.wait()


def _params(mib=64):
    return pltpu.CompilerParams(has_side_effects=True, vmem_limit_bytes=mib * 2**20 - 65536)


def solution(mesh):
    tile = P(None, 'h', 'w', None)
    cnt = float(TH * TW * 16 * (C // GROUPS))
    sds = jax.ShapeDtypeStruct
    V = pltpu.VMEM

    def body(x, w1, gamma, beta, w2, g):
        x2, g2 = x.reshape(PIX, C), g.reshape(PIX, C)
        w1r, w2r = w1.reshape(3, 3 * C, C), w2.reshape(3, 3 * C, C)
        ga, be = gamma.reshape(1, C), beta.reshape(1, C)
        tile, flip, wide, wts = sds((PIX, C), BF), sds((C, PIX), BF), sds((10 * TW, 3 * C), BF), sds((3, 3 * C, C), BF)
        dw = sds((3, 3, C, C), F32)
        vm = lambda l: [V(a.shape, a.dtype) for a in l]
        sums = [V((8, C), F32)]
        sems = [DMA((16,)), DMA((16,)), DMA((8,)), DMA((2,))]
        gcat, a, z, zt, xt, stat = pl.pallas_call(
            lambda *r: _k1(cnt, *r),
            out_shape=[wide, tile, tile, flip, flip, sds((8, C), F32)],
            in_specs=[ANY] * 3 + [VM] * 2, out_specs=[ANY] * 5 + [VM],
            scratch_shapes=vm((tile, tile, wts, wide, wide, tile, tile, flip, flip)) + sums + [V((16, 8, 128), F32)] + sems + _halo_scratch() * 2,
            compiler_params=_params(), name='k1')(x2, w1r, g2, ga, be)
        piece = sds((3, 3, EIGHTH, C), F32)
        dw2, y, dx, f1, t = pl.pallas_call(
            lambda *r: _k2(cnt, *r),
            out_shape=[dw, tile, tile, piece, sds((8, C), F32)],
            in_specs=[ANY] * 3 + [VM] * 3 + [ANY] * 6, out_specs=[ANY] * 3 + [VM] * 2,
            scratch_shapes=vm((wide, flip, tile, wts, tile)) + sums + [V((16, 16, 128), F32)] + sems + vm((piece,))
            + _halo_scratch() * 2 + _rs_buffers() + _rs_scratch() * 2 + _ag_scratch(),
            compiler_params=_params(), name='k2')(gcat, zt, a, stat, ga, be, w2r, w1r, xt, x2, z, g2)
        dw1 = pl.pallas_call(
            _k3, out_shape=dw, in_specs=[VM], out_specs=VM,
            scratch_shapes=_ag_scratch(),
            compiler_params=_params(2), name='k3')(f1)
        dw1, dw2, y, dx = pl.pallas_call(
            _k4, out_shape=[dw, dw, tile, tile], in_specs=[VM] * 4, out_specs=[ANY] * 4,
            scratch_shapes=sems[2:3], compiler_params=pltpu.CompilerParams(vmem_limit_bytes=2**20), name='k4')(dw1, dw2, y, dx)
        return y.reshape(x.shape), dx.reshape(x.shape), dw1, dw2, t[0], t[1]

    return jax.shard_map(body, mesh=mesh, in_specs=(tile, P(), P(), P(), P(), tile), out_specs=(tile, tile, P(), P(), P(), P()), check_vma=False)
```
